32 devices in a mesh: dp: 8 (over y, x, core), expert: 4 (over z).
Axes of the slice: x: 2, y: 2, z: 4, core: 2. Of those that a mesh axis runs over, the one named last changes fastest.
Arguments:
- tokens_in: bfloat16 [4096, 2048], P(('dp', 'expert')), may hold values from -6 to 6
- out_grad: bfloat16 [4096, 2048], P(('dp', 'expert')), may hold values from -3 to 3
- expert_ids: int32 [4096, 8], P(('dp', 'expert')), may hold values from 0 to 127, all different within a row; in each aligned block of 128 rows (0 to 127, 128 to 255, ...) at most 16 rows name the same one
- rest_scores: float32 [4096, 8], P(('dp', 'expert')), may hold values from -60 to 60
- router_weight: bfloat16 [2048, 128], replicated, may hold values from -0.125 to 0.125
- down_weight: bfloat16 [4, 768, 2048], P('expert'), may hold values from -0.125 to 0.125
- saved_hidden: bfloat16 [8, 4, 4, 16, 768], P('dp', 'expert'), may hold values from -6 to 6
Outputs:
- token_grad: bfloat16 [4096, 2048], P(('dp', 'expert'))
- router_grad: float32 [2048, 128], P('dp', 'expert')
- down_grad: float32 [4, 768, 2048], P('expert', 'dp')
- hidden_grad: bfloat16 [8, 4, 4, 16, 768], P('dp', 'expert')
The draws below stay inside these ranges and needn't reach their ends.
Inputs may be any that keep to these rules, and one draw needn't show every extreme that they name: `expert_ids`: each row names 8 different experts; among the 128 tokens of one device no expert is named more than 16 times, a bound that some block reaches.
All inputs are finite; a program needn't handle non-finite values.
Results may differ from the reference program's by a relative error of at most 0.024.
Values may be sent and summed in bfloat16 or wider, within the bound.
A program may use at most 64 MiB of HBM per device.

```python
import math
import jax
import jax.numpy as jnp
import numpy as np
from jax import lax

D = 2048
FF = 768
EXPERTS = 128
TOPK = 8
TOK_DEV = 128
CAP = 16
WIN = 4
TOKENS = 4096
N_DP = 8
N_EXPERT = 4


def level_of(stream_key, shape, split, low, top_value):
    factor_of = 1.0
    for axis_at, blocks in split:
        steps = jax.random.uniform(jax.random.fold_in(jax.random.fold_in(stream_key, 6), axis_at), (blocks,), jnp.float32, low / len(split), top_value / len(split))
        factor_of = factor_of * jnp.repeat(jnp.exp(steps), shape[axis_at] // blocks).reshape((-1,) + (1,) * (len(shape) - 1 - axis_at))
    return factor_of


def routed_block(key, own, number, rows, count, top, limit, lean):
    order = jax.random.permutation(key, count)
    crowded, usual = shares(count, rows * top, limit, lean, True), shares(count, rows * top, limit, lean, False)
    places = jnp.arange(count)

    def named(sizes, offset_by):
        used = int((sizes > 0).sum())
        fixed = max(1, used // 4)
        passed = fixed + (places - fixed + offset_by * (used - fixed)) % max(1, count - fixed)
        return jnp.zeros((count,), jnp.int32).at[order[jnp.where(places < fixed, places, passed)]].set(jnp.asarray(sizes, jnp.int32))

    sizes = jnp.where(number % 4 == 0, named(crowded, number // 4), named(usual, number - number // 4 - 1))
    mixed = jax.random.permutation(jax.random.fold_in(own, 3), count)
    source_of, sink = mixed[0:count // 2 * 2:2], mixed[1:count // 2 * 2:2]
    room = jnp.minimum(sizes[source_of] - 1, limit - sizes[sink]) // 2
    room = jnp.where((source_of == order[0]) | (sink == order[0]) | (sizes[sink] == 0), 0, jnp.maximum(room, 0))
    passed = jax.random.randint(jax.random.fold_in(own, 4), (count // 2,), 0, 1 << 20) % (room + 1)
    sizes = sizes.at[source_of].add(-passed).at[sink].add(passed)
    items = jnp.searchsorted(jnp.cumsum(sizes), jnp.arange(rows * top), side="right").astype(jnp.int32)
    grid = items.reshape(top, rows).T
    grid = grid[jax.random.permutation(jax.random.fold_in(own, 1), rows)]
    offset_by = jax.random.randint(jax.random.fold_in(own, 2), (rows, 1), 0, top)
    return jnp.take_along_axis(grid, (jnp.arange(top)[None, :] + offset_by) % top, axis=1)


def shares(number_of, total, bound, slope, full):
    portions = [(1 << 20) // math.isqrt(grade ** slope) + 1 for grade in range(1, number_of + 1)]
    largest = bound if full else min(bound, max(-(-total // number_of), total * portions[0] // sum(portions)))
    least = 1 if total - largest >= number_of - 1 else 0
    holding, rest = [largest] + [least] * (number_of - 1), total - largest - least * (number_of - 1)
    while rest > 0:
        free = [i for i in range(1, number_of) if holding[i] < largest] or [i for i in range(1, number_of) if holding[i] < bound]
        pool, remaining = sum([portions[i] for i in free]), rest
        for i in free:
            addition = min(bound - holding[i], max(1, remaining * portions[i] // pool), rest)
            holding[i] = holding[i] + addition
            rest = rest - addition
    return np.array(holding)


def bell_draw(own_key, shape, scale, limit, shards=(), kind=jnp.bfloat16):
    entries = jax.random.normal(own_key, shape, jnp.float32) * scale
    if len(shards) > 0:
        entries = level_of(own_key, shape, shards, -0.22, 0.18) * entries
    return jnp.clip(entries, min=-limit, max=limit).astype(kind)


def setup_inputs(seed: int = 0) -> dict:
    streams_of = jax.random.split(jax.random.key(seed), 8)
    tokens_in = bell_draw(streams_of[0], (TOKENS, D), 1.0, 6.0, ((0, 32),))
    out_grad = bell_draw(streams_of[1], (TOKENS, D), 0.5, 3.0, ((0, 32),))
    expert_ids_keys = jax.random.split(jax.random.fold_in(streams_of[2], 1), TOKENS // TOK_DEV)
    expert_ids_turns = jax.random.permutation(jax.random.fold_in(streams_of[2], 3), TOKENS // TOK_DEV)
    expert_ids = jax.vmap(lambda own, number: routed_block(jax.random.fold_in(streams_of[2], 2), own, number, TOK_DEV, EXPERTS, TOPK, CAP, 2))(expert_ids_keys, expert_ids_turns).reshape((TOKENS, TOPK))
    rest_scores = bell_draw(streams_of[3], (TOKENS, TOPK), 10.0, 60.0, ((0, 32),), jnp.float32)
    router_weight = bell_draw(streams_of[4], (D, EXPERTS), D ** -0.5, 0.125)
    down_weight = bell_draw(streams_of[5], (WIN, FF, D), D ** -0.5, 0.125, ((0, 4),))
    saved_hidden = bell_draw(streams_of[6], (N_DP, WIN, N_EXPERT, CAP, FF), 1.0, 6.0, ((0, 8), (1, 4)))
    return {"tokens_in": tokens_in, "out_grad": out_grad, "expert_ids": expert_ids, "rest_scores": rest_scores, "router_weight": router_weight, "down_weight": down_weight, "saved_hidden": saved_hidden}


def slot_layout(ids_block, window, capacity):
    hit_mask = (ids_block[:, :, None] == jnp.arange(window, dtype=jnp.int32)[None, None, :]).astype(jnp.int32)
    chosen = jnp.sum(hit_mask, axis=1)
    before = jnp.cumsum(chosen, axis=0) - chosen
    placed = (chosen[None, :, :] == 1) & (before[None, :, :] == jnp.arange(capacity, dtype=jnp.int32)[:, None, None])
    slot_table = jnp.transpose(placed, (2, 0, 1)).astype(jnp.float32)
    return slot_table, hit_mask.astype(jnp.float32)


def reference(tokens_in, out_grad, expert_ids, rest_scores, router_weight, down_weight, saved_hidden):
    window = N_EXPERT
    capacity = saved_hidden.shape[3]
    sources = N_EXPERT
    logits = jnp.dot(tokens_in, router_weight, preferred_element_type=jnp.float32)
    picked = jnp.take_along_axis(logits, expert_ids, axis=1)
    gate_sel = jax.nn.softmax(picked, axis=1)
    grad_rows = out_grad.reshape(N_DP, sources, TOK_DEV, D)
    ids_rows = expert_ids.reshape(N_DP, sources, TOK_DEV, TOPK)
    gate_rows = gate_sel.reshape(N_DP, sources, TOK_DEV, TOPK)
    weight_f = down_weight.astype(jnp.float32)

    def one_row(total, packed):
        grad_blk, ids_blk, gate_blk, hidden_blk = packed
        slot_table, hit_mask = jax.vmap(lambda ids: slot_layout(ids, window, capacity))(ids_blk)
        gate_each = jnp.einsum('stkw,stk->stw', hit_mask, gate_blk)
        position = jnp.sum(slot_table * jnp.arange(TOK_DEV, dtype=jnp.float32), axis=-1).astype(jnp.int32)
        filled = jnp.sum(slot_table, axis=-1)
        sent_grad = jax.vmap(lambda grads, where_at: grads[where_at])(grad_blk, position)
        sent_grad = sent_grad * filled[..., None].astype(jnp.bfloat16)
        sent_gate = jnp.einsum('swct,stw->swc', slot_table, gate_each).astype(jnp.bfloat16)
        got_grad = jnp.transpose(sent_grad, (1, 0, 2, 3)).astype(jnp.float32)
        got_gate = jnp.transpose(sent_gate, (1, 0, 2)).astype(jnp.float32)
        raw_grad = jnp.einsum('wscd,wfd->wscf', got_grad, weight_f)
        hidden_f = hidden_blk.astype(jnp.float32)
        hid_grad = (got_gate[..., None] * raw_grad).astype(jnp.bfloat16)
        scores = jnp.sum(raw_grad * hidden_f, axis=-1)
        scaled = lax.optimization_barrier((got_gate[..., None] * got_grad).astype(jnp.bfloat16)).astype(jnp.float32)
        partial_value = jnp.einsum('wscf,wscd->wfd', hidden_f, scaled)
        partial_value = lax.optimization_barrier(partial_value.astype(jnp.bfloat16)).astype(jnp.float32)
        per_token = jnp.einsum('swct,wsc->stw', slot_table, scores)
        score_tok = jnp.einsum('stkw,stw->stk', hit_mask, per_token)
        return total + partial_value, (hid_grad, score_tok)

    start_total = jnp.zeros((window, FF, D), jnp.float32)
    down_grad, (hidden_grad, score_rows) = lax.scan(one_row, start_total, (grad_rows, ids_rows, gate_rows, saved_hidden))
    score_all = score_rows.reshape(TOKENS, TOPK)
    score_all = jnp.where(expert_ids < window, score_all, rest_scores)
    mean_part = jnp.sum(gate_sel * score_all, axis=1, keepdims=True)
    logit_sel = gate_sel * (score_all - mean_part)
    row_index = jnp.arange(TOKENS, dtype=jnp.int32)[:, None]
    logit_grad = jnp.zeros((TOKENS, EXPERTS), jnp.float32).at[row_index, expert_ids].add(logit_sel)
    logit_bf = logit_grad.astype(jnp.bfloat16)
    router_grad = jnp.dot(tokens_in.T, logit_bf, preferred_element_type=jnp.float32)
    token_grad = jnp.dot(logit_bf, router_weight.T, preferred_element_type=jnp.float32).astype(jnp.bfloat16)
    return token_grad, router_grad, down_grad, hidden_grad
```

```python
import functools
import jax
import jax.numpy as jnp
from jax import lax
from jax.experimental import pallas as pl
from jax.experimental.pallas import tpu as pltpu
from jax.sharding import PartitionSpec as P


def slot_layout(ids_block, window, capacity):
    hit_mask = (ids_block[:, :, None] == jnp.arange(window, dtype=jnp.int32)[None, None, :]).astype(
        jnp.int32
    )
    chosen = jnp.sum(hit_mask, axis=1)
    before = jnp.cumsum(chosen, axis=0) - chosen
    placed = (chosen[None, :, :] == 1) & (
        before[None, :, :] == jnp.arange(capacity, dtype=jnp.int32)[:, None, None]
    )
    slot_table = jnp.transpose(placed, (2, 0, 1)).astype(jnp.float32)
    return (slot_table, hit_mask.astype(jnp.float32))


def shards(tokens_in, out_grad, expert_ids, rest_scores, router_weight, down_weight, saved_hidden):
    window = lax.axis_size("expert")
    capacity = saved_hidden.shape[3]
    sources = saved_hidden.shape[2]
    hidden_units = saved_hidden.shape[4]
    width = out_grad.shape[1]
    scored = router_weight.shape[1]
    logits = jnp.dot(tokens_in, router_weight, preferred_element_type=jnp.float32)
    all_mask = (
        expert_ids[:, :, None] == jnp.arange(scored, dtype=jnp.int32)[None, None, :]
    ).astype(jnp.float32)
    picked = jnp.sum(all_mask * logits[:, None, :], axis=2)
    gate_sel = jax.nn.softmax(picked, axis=1)
    slot_table, hit_mask = slot_layout(expert_ids, window, capacity)
    gate_each = jnp.einsum("tkw,tk->tw", hit_mask, gate_sel)
    sent_grad = jnp.einsum(
        "wct,td->wcd", slot_table.astype(jnp.bfloat16), out_grad, preferred_element_type=jnp.float32
    ).astype(jnp.bfloat16)
    sent_gate = jnp.einsum("wct,tw->wc", slot_table, gate_each).astype(jnp.bfloat16)
    got_grad, got_gate = (
        lax.all_to_all(sent_grad, "expert", split_axis=0, concat_axis=0, tiled=True),
        lax.all_to_all(sent_gate, "expert", split_axis=0, concat_axis=0, tiled=True),
    )
    slot_rows = got_grad.reshape(sources * capacity, width)
    gate_flat = got_gate.reshape(sources * capacity).astype(jnp.float32)
    weight_now = down_weight[0]
    raw_grad = lax.dot_general(
        slot_rows, weight_now, (((1,), (1,)), ((), ())), preferred_element_type=jnp.float32
    )
    hidden_flat = saved_hidden[0, 0].reshape(sources * capacity, hidden_units)
    hid_grad = (gate_flat[:, None] * raw_grad).astype(jnp.bfloat16)
    scores = jnp.sum(raw_grad * hidden_flat.astype(jnp.float32), axis=1).reshape(sources, capacity)
    scaled = (gate_flat[:, None] * slot_rows.astype(jnp.float32)).astype(jnp.bfloat16)
    down_grad = lax.psum_scatter(
        lax.dot_general(
            hidden_flat, scaled, (((0,), (0,)), ((), ())), preferred_element_type=jnp.float32
        ).astype(jnp.bfloat16),
        "dp",
        scatter_dimension=0,
        tiled=True,
    ).astype(jnp.float32)
    returned = lax.all_to_all(scores, "expert", split_axis=0, concat_axis=0, tiled=True)
    per_token = jnp.einsum("wct,wc->tw", slot_table, returned)
    score_tok = jnp.einsum("tkw,tw->tk", hit_mask, per_token)
    score_all = jnp.where(expert_ids < window, score_tok, rest_scores)
    mean_part = jnp.sum(gate_sel * score_all, axis=1, keepdims=True)
    logit_sel = gate_sel * (score_all - mean_part)
    logit_bf = jnp.einsum("tke,tk->te", all_mask, logit_sel).astype(jnp.bfloat16)
    summed_rows = lax.psum_scatter(
        lax.dot_general(
            tokens_in, logit_bf, (((0,), (0,)), ((), ())), preferred_element_type=jnp.float32
        ).astype(jnp.bfloat16),
        "dp",
        scatter_dimension=0,
        tiled=True,
    )
    router_grad = lax.psum_scatter(summed_rows, "expert", scatter_dimension=1, tiled=True).astype(
        jnp.float32
    )
    token_grad = lax.dot_general(
        logit_bf, router_weight, (((1,), (1,)), ((), ())), preferred_element_type=jnp.float32
    ).astype(jnp.bfloat16)
    hidden_grad = hid_grad.reshape(1, 1, sources, capacity, hidden_units)
    return (token_grad, router_grad, down_grad[None], hidden_grad)


MESH = pl.DeviceIdType.MESH
F32, BF16 = jnp.float32, jnp.bfloat16


def flip(index, mask):
    out = 0
    for bit in (1, 2, 4):
        digit = lax.rem(lax.div(index, bit), 2)
        out = out + bit * ((1 - digit) if mask & bit else digit)
    return out


def rows_times(a, b):
    return lax.dot_general(a, b, (((1,), (1,)), ((), ())), preferred_element_type=F32)


def times(a, b):
    return lax.dot_general(a, b, (((1,), (0,)), ((), ())), preferred_element_type=F32)


def layer_kernel(
    nd, nz, cap,
    tok_h, grad_h, ids_h, rest_h, rw_h, w_h, hid_h,
    token_o, router_o, down_o, hidden_o,
    tok, grad, ids, rest, rw, weight, hid,
    blk, gat, y, gate_s, gate_r, ret_s, ret_r, tok_all, info_s, info_all, sc_s, sc_all,
    gate_all, base_all, hg_s, hg_all, rg_s, rg_r,
    load_sem, send_sem, recv_sem, disp_r, near_r, in_r,
):
    me = lax.axis_index("dp")
    mz = lax.axis_index("expert")
    tokens, width = tok.shape
    experts = rw.shape[1]
    slots = nz * cap
    hidden_units = hid.shape[1]
    own_cols = width // nd

    loads = []
    for i, (src, dst) in enumerate(
        ((ids_h, ids), (grad_h, grad), (tok_h, tok), (rw_h, rw), (rest_h, rest), (hid_h, hid), (w_h, weight))
    ):
        loads.append(pltpu.make_async_copy(src, dst, load_sem.at[i]))
        loads[-1].start()
    ld_ids, ld_grad, ld_tok, ld_rw, ld_rest, ld_hid, ld_w = loads

    disp_s, gsem_s, ag_s, tk_s, rs_s, in_s, st_s, hs_s, zr_s = [send_sem.at[i] for i in range(9)]
    gsem_r, tk_r, rs_r, ina_r, st_r, hs_r, zr_r, core_r, last_r = [recv_sem.at[i] for i in range(9)]
    peers = [flip(me, p) for p in range(nd)]
    half = lax.div(mz, 2)
    near = [mz, mz + 1 - 2 * lax.rem(mz, 2), 2 - half, 3 - 3 * half]
    barrier = pltpu.get_barrier_semaphore()
    for p in range(1, nd):
        pl.semaphore_signal(barrier, inc=1, device_id=(peers[p], mz), device_id_type=MESH)
    for k in range(1, nz):
        pl.semaphore_signal(barrier, inc=1, device_id=(me, near[k]), device_id_type=MESH)

    def send(src, dst, s_sem, r_sem, device):
        pltpu.make_async_remote_copy(
            src_ref=src, dst_ref=dst, send_sem=s_sem, recv_sem=r_sem, device_id=device, device_id_type=MESH
        ).start()

    def arrived(ref, r_sem):
        pltpu.make_async_copy(ref, ref, r_sem).wait()

    e_row = lax.broadcasted_iota(jnp.int32, (experts, tokens), 0)
    ld_ids.wait()
    idv = ids[...]
    topk = idv.shape[0]
    hits = [idv[k : k + 1, :] == e_row for k in range(topk)]
    mask = hits[0]
    for k in range(1, topk):
        mask = mask | hits[k]
    t_row = lax.broadcasted_iota(jnp.int32, (tokens, tokens), 0)
    t_col = lax.broadcasted_iota(jnp.int32, (tokens, tokens), 1)
    earlier = jnp.where(t_row < t_col, 1.0, 0.0).astype(BF16)
    chosen = jnp.where(mask, 1.0, 0.0)
    place = jnp.where(mask, times(chosen.astype(BF16), earlier), -1.0)
    c_row = lax.broadcasted_iota(jnp.int32, (cap, tokens), 0).astype(F32)
    tables = [jnp.where(place[e : e + 1, :] == c_row, 1.0, 0.0) for e in range(nz)]
    table = jnp.concatenate(tables, axis=0).astype(BF16)

    ld_grad.wait()
    blk[...] = times(table, grad[...]).astype(BF16).reshape(blk.shape)
    gat[me, mz] = blk[mz]

    pl.semaphore_wait(barrier, nd - 1 + nz - 1)
    for k in Z_ORDER:
        send(blk.at[near[k]], gat.at[me, mz], disp_s, disp_r.at[mz], (me, near[k]))

    def spread(ref, k, origin, target):
        from_p = origin ^ target
        if from_p % 2 == 0:
            r_sem = near_r.at[k, from_p // 2]
        else:
            r_sem = last_r if from_p == 7 else core_r
        send(ref, ref, ag_s, r_sem, (peers[target], mz))

    def landed(k):
        arrived(gat.at[me, near[k]], disp_r.at[near[k]])

    def spread_own(k):
        ref = gat.at[me, near[k]]
        for target in (2, 4, 1):
            spread(ref, k, 0, target)

    def relay_near(k):
        via = 2 if k % 2 == 0 else 4
        for origin in (via, 6 - via):
            ref = gat.at[peers[origin], near[k]]
            arrived(ref, near_r.at[k, origin // 2])
            if origin == via:
                spread(ref, k, origin, 6 - via)
            spread(ref, k, origin, 1)

    def relay_far(k):
        ref = gat.at[peers[6], near[k]]
        arrived(ref, near_r.at[k, 3])
        spread(ref, k, 6, 1)

    spread_own(0)

    ld_tok.wait()
    ld_rw.wait()
    logits = times(tok[...], rw[...]).T
    low = jnp.where(mask, logits, -3.0e38)
    raised = jnp.where(mask, jnp.exp(low - jnp.max(low, axis=0, keepdims=True)), 0.0)
    gate = raised / jnp.sum(raised, axis=0, keepdims=True)
    for k in range(topk):
        info_s[k : k + 1, :] = jnp.sum(jnp.where(hits[k], gate, 0.0), axis=0, keepdims=True)
    ld_rest.wait()
    restv = rest[...]
    info_s[topk : 2 * topk, :] = restv
    info_s[2 * topk : 3 * topk, :] = idv.astype(F32)
    for e in range(nz):
        one = jnp.sum(tables[e] * gate[e : e + 1, :], axis=1, keepdims=True)
        gate_s[e] = jnp.broadcast_to(one, (cap, experts)).astype(BF16)
    gate_r[mz] = gate_s[mz]
    for k in range(1, nz):
        send(gate_s.at[near[k]], gate_r.at[mz], gsem_s, gsem_r, (me, near[k]))
    for p in (6, 2, 4, 1):
        send(info_s, info_all.at[me], in_s, in_r.at[p // 2] if p > 1 else ina_r, (peers[p], mz))
    for p in TOKEN_ORDER:
        cols = pl.ds(pl.multiple_of(peers[p] * own_cols, own_cols), own_cols)
        send(tok.at[:, cols], tok_all.at[me], tk_s, tk_r, (peers[p], mz))

    ld_hid.wait()
    ld_w.wait()
    y[...] = times(hid[...], weight[...]).reshape(y.shape)

    outside = e_row >= nz

    def expand(j, g, r):
        r = jnp.where(outside, r, 0.0)
        gate_all[j] = g
        base_all[j] = g * (r - jnp.sum(g * r, axis=0, keepdims=True))

    rest_all = jnp.where(hits[0], restv[0:1, :], 0.0)
    for k in range(1, topk):
        rest_all = jnp.where(hits[k], restv[k : k + 1, :], rest_all)
    expand(me, gate, rest_all)
    tok_all[me] = tok[:, pl.ds(pl.multiple_of(me * own_cols, own_cols), own_cols)]

    def score_of(k):
        score = jnp.sum(gat[me, near[k]].astype(F32) * y[near[k]], axis=1, keepdims=True)
        target = ret_s if k else ret_r
        target[near[k]] = jnp.broadcast_to(score, (cap, tokens))
        if k:
            send(ret_s.at[near[k]], ret_r.at[mz], rs_s, rs_r, (me, near[k]))

    score_of(0)
    landed(1)
    score_of(1)
    spread_own(1)
    relay_near(0)
    landed(2)
    score_of(2)
    spread_own(2)
    landed(3)
    score_of(3)
    if not LATE_SPREAD:
        spread_own(3)
    arrived(gate_r.at[1:nz], gsem_r)
    slot_g = gate_r[...].reshape(slots, experts)[:, 0:1].astype(F32)
    hidden_f = hid[...].astype(F32)
    scaled_t = (slot_g * hidden_f).T.astype(BF16)
    hg_s[...] = scaled_t.reshape(hg_s.shape)
    hg_all[me] = hg_s[me]

    for p in (2, 4, 6):
        ref = info_all.at[peers[p]]
        arrived(ref, in_r.at[p // 2])
        send(ref, ref, in_s, ina_r, (peers[1], mz))
    e_rowf = e_row.astype(F32)
    for p in (2, 4, 6, 1, 3, 5, 7):
        j = peers[p]
        if p == 1:
            arrived(info_all.at[0:4], ina_r)
        g = jnp.zeros((experts, tokens), F32)
        r = g
        for k in range(topk):
            hit = info_all[j, 2 * topk + k : 2 * topk + k + 1, :] == e_rowf
            g = jnp.where(hit, info_all[j, k : k + 1, :], g)
            r = jnp.where(hit, info_all[j, topk + k : topk + k + 1, :], r)
        expand(j, g, r)

    arrived(ret_r.at[1:nz], rs_r)
    for e in range(nz):
        sc_s[e : e + 1, :] = jnp.sum(tables[e] * ret_r[e], axis=0, keepdims=True)
    for p in TOKEN_ORDER:
        send(sc_s, sc_all.at[me], st_s, st_r, (peers[p], mz))
    if LATE_SPREAD:
        spread_own(3)
    for p in TOKEN_ORDER:
        send(hg_s.at[peers[p]], hg_all.at[me], hs_s, hs_r, (peers[p], mz))

    def logit_grad(j, score):
        g = gate_all[j]
        mean = jnp.sum(g[0:nz, :] * score, axis=0, keepdims=True)
        late = base_all[j] - g * mean
        for e in range(nz):
            late = late + jnp.where(e_row == e, g * score[e : e + 1, :], 0.0)
        return late

    def hidden_part(n, parts):
        step = hidden_units // parts
        raw = rows_times(gat[me].reshape(slots, width), weight[n * step : (n + 1) * step, :])
        hidden_o[:, n * step : (n + 1) * step] = (slot_g * raw).astype(BF16)

    own_grad = logit_grad(me, sc_s[0:nz, :])
    token_o[...] = rows_times(own_grad.T.astype(BF16), rw[...]).astype(BF16)
    relay_near(1)
    relay_near(2)
    relay_far(0)
    relay_near(3)
    arrived(sc_all.at[1:nd], st_r)
    grads = [own_grad.astype(BF16)]
    for p in range(1, nd):
        grads.append(logit_grad(peers[p], sc_all[peers[p], 0:nz, :]).astype(BF16))
    arrived(tok_all.at[1:nd], tk_r)
    lhs = jnp.concatenate(grads, axis=1)
    rhs = jnp.concatenate([tok_all[peers[p]] for p in range(nd)], axis=0)
    partial = times(lhs, rhs)
    rg_s[...] = partial.reshape(rg_s.shape).astype(BF16)
    rg_r[mz] = rg_s[mz]
    for k in Z_ORDER:
        send(rg_s.at[near[k]], rg_r.at[mz], zr_s, zr_r, (me, near[k]))
    hidden_part(0, 3)
    relay_far(1)
    hidden_part(1, 3)
    relay_far(2)
    hidden_part(2, 3)
    relay_far(3)

    arrived(hg_all.at[1:nd], hs_r)
    arrived(gat.at[0:3], core_r)

    def down_part(group, first):
        lhs = jnp.concatenate([hg_all[peers[p]] for p in group], axis=1)
        step = width // 4
        for n in range(4):
            cols = slice(n * step, (n + 1) * step)
            rhs = jnp.concatenate([gat[peers[p], :, :, cols].reshape(slots, step) for p in group], axis=0)
            part = times(lhs, rhs)
            down_o[:, cols] = part if first else down_o[:, cols] + part

    down_part(range(0, 4), True)
    arrived(gat.at[0], last_r)
    down_part(range(4, 8), False)

    arrived(rg_r.at[1:nz], zr_r)
    total = rg_r[0].astype(F32)
    for k in range(1, nz):
        total = total + rg_r[k].astype(F32)
    router_o[...] = total
    arrived(blk.at[1:nz], disp_s)
    arrived(gate_s.at[1:nz], gsem_s)
    arrived(gat.at[1:nd], ag_s)
    arrived(tok_all.at[1:nd], tk_s)
    arrived(ret_s.at[1:nz], rs_s)
    arrived(info_all.at[1:nd], in_s)
    arrived(sc_all.at[1:nd], st_s)
    arrived(hg_s.at[1:nd], hs_s)
    arrived(rg_s.at[1:nz], zr_s)


def out_kernel(count, *refs):
    sem = refs[-1]
    copies = [pltpu.make_async_copy(refs[i], refs[count + i], sem.at[i]) for i in range(count)]
    for copy in copies:
        copy.start()
    for copy in copies:
        copy.wait()


def hand_out(results):
    count = len(results)
    return pl.pallas_call(
        functools.partial(out_kernel, count),
        out_shape=tuple(jax.ShapeDtypeStruct(r.shape, r.dtype) for r in results),
        in_specs=[pl.BlockSpec(memory_space=pl.ANY)] * count,
        out_specs=(pl.BlockSpec(memory_space=pltpu.HBM),) * count,
        scratch_shapes=[pltpu.SemaphoreType.DMA((count,))],
        compiler_params=pltpu.CompilerParams(vmem_limit_bytes=2**20),
    )(*results)


VMEM_BYTES = 67043328
TOKEN_ORDER = (6, 7, 2, 4, 3, 5, 1)
Z_ORDER = (3, 2, 1)
LATE_SPREAD = True


def fused(nd, nz, tokens_in, out_grad, expert_ids, rest_scores, router_weight, down_weight, saved_hidden):
    cap, hidden_units = saved_hidden.shape[3], saved_hidden.shape[4]
    sources = saved_hidden.shape[2]
    tokens, width = tokens_in.shape
    experts = router_weight.shape[1]
    topk = expert_ids.shape[1]
    slots = sources * cap
    own_rows, own_cols, own_exp = hidden_units // nd, width // nd, experts // nz
    vm, dma = pltpu.VMEM, pltpu.SemaphoreType.DMA
    scratch = [
        vm((tokens, width), BF16), vm((tokens, width), BF16),
        vm(expert_ids.shape[::-1], jnp.int32), vm(rest_scores.shape[::-1], F32),
        vm((width, experts), BF16), vm((hidden_units, width), BF16), vm((slots, hidden_units), BF16),
        vm((nz, cap, width), BF16), vm((nd, nz, cap, width), BF16), vm((nz, cap, width), F32),
        vm((nz, cap, experts), BF16), vm((nz, cap, experts), BF16),
        vm((nz, cap, tokens), F32), vm((nz, cap, tokens), F32),
        vm((nd, tokens, own_cols), BF16),
        vm((3 * topk, tokens), F32), vm((nd, 3 * topk, tokens), F32),
        vm((nz, tokens), F32), vm((nd, nz, tokens), F32),
        vm((nd, experts, tokens), F32), vm((nd, experts, tokens), F32),
        vm((nd, own_rows, slots), BF16), vm((nd, own_rows, slots), BF16),
        vm((nz, own_exp, own_cols), BF16), vm((nz, own_exp, own_cols), BF16),
        dma((7,)), dma((9,)), dma((9,)), dma((nz,)), dma((nz, nz)), dma((nz,)),
    ]
    vm_spec = pl.BlockSpec(memory_space=pltpu.VMEM)
    held = 2 * tokens * width + 4 * own_exp * own_cols + 4 * own_rows * width + 2 * slots * hidden_units
    token_grad, router_grad, down_grad, hidden_grad = pl.pallas_call(
        functools.partial(layer_kernel, nd, nz, cap),
        out_shape=(
            pltpu.VMEM((tokens, width), BF16),
            pltpu.VMEM((own_exp, own_cols), F32),
            pltpu.VMEM((own_rows, width), F32),
            pltpu.VMEM((slots, hidden_units), BF16),
        ),
        in_specs=[pl.BlockSpec(memory_space=pltpu.HBM)] * 7,
        out_specs=(vm_spec,) * 4,
        scratch_shapes=scratch,
        compiler_params=pltpu.CompilerParams(
            collective_id=0, has_side_effects=True, vmem_limit_bytes=VMEM_BYTES - held
        ),
    )(
        tokens_in, out_grad, expert_ids.T, rest_scores.T, router_weight,
        down_weight[0], saved_hidden.reshape(slots, hidden_units),
    )
    results = (token_grad, router_grad, down_grad, hidden_grad)
    token_grad, router_grad, down_grad, hidden_grad = hand_out(results)
    return token_grad, router_grad.T, down_grad[None], hidden_grad.reshape(saved_hidden.shape)


def body(nd, nz, *args):
    tokens_in, saved_hidden, router_weight = args[0], args[6], args[4]
    slots = saved_hidden.shape[2] * saved_hidden.shape[3]
    gathered = nd * slots * tokens_in.shape[1] * 2
    fits = nd == 8 and gathered <= 16 * 2**20 and saved_hidden.shape[2] == nz
    fits = fits and nz == 4 and (saved_hidden.shape[4] // nd) % 16 == 0
    if fits:
        return fused(nd, nz, *args)
    return shards(*args)


def solution(mesh):
    sizes = dict(mesh.shape)
    return jax.shard_map(
        functools.partial(body, sizes["dp"], sizes["expert"]),
        mesh=mesh,
        in_specs=(
            P(("dp", "expert"), None),
            P(("dp", "expert"), None),
            P(("dp", "expert"), None),
            P(("dp", "expert"), None),
            P(),
            P("expert", None, None),
            P("dp", "expert", None, None, None),
        ),
        out_specs=(
            P(("dp", "expert"), None),
            P("dp", "expert"),
            P("expert", "dp", None),
            P("dp", "expert", None, None, None),
        ),
        check_vma=False,
    )
```

```python
import functools
import jax
import jax.numpy as jnp
from jax import lax
from jax.experimental import pallas as pl
from jax.experimental.pallas import tpu as pltpu
from jax.sharding import PartitionSpec as P


def slot_layout(ids_block, window, capacity):
    hit_mask = (ids_block[:, :, None] == jnp.arange(window, dtype=jnp.int32)[None, None, :]).astype(
        jnp.int32
    )
    chosen = jnp.sum(hit_mask, axis=1)
    before = jnp.cumsum(chosen, axis=0) - chosen
    placed = (chosen[None, :, :] == 1) & (
        before[None, :, :] == jnp.arange(capacity, dtype=jnp.int32)[:, None, None]
    )
    slot_table = jnp.transpose(placed, (2, 0, 1)).astype(jnp.float32)
    return (slot_table, hit_mask.astype(jnp.float32))


def shards(tokens_in, out_grad, expert_ids, rest_scores, router_weight, down_weight, saved_hidden):
    window = lax.axis_size("expert")
    capacity = saved_hidden.shape[3]
    sources = saved_hidden.shape[2]
    hidden_units = saved_hidden.shape[4]
    width = out_grad.shape[1]
    scored = router_weight.shape[1]
    logits = jnp.dot(tokens_in, router_weight, preferred_element_type=jnp.float32)
    all_mask = (
        expert_ids[:, :, None] == jnp.arange(scored, dtype=jnp.int32)[None, None, :]
    ).astype(jnp.float32)
    picked = jnp.sum(all_mask * logits[:, None, :], axis=2)
    gate_sel = jax.nn.softmax(picked, axis=1)
    slot_table, hit_mask = slot_layout(expert_ids, window, capacity)
    gate_each = jnp.einsum("tkw,tk->tw", hit_mask, gate_sel)
    sent_grad = jnp.einsum(
        "wct,td->wcd", slot_table.astype(jnp.bfloat16), out_grad, preferred_element_type=jnp.float32
    ).astype(jnp.bfloat16)
    sent_gate = jnp.einsum("wct,tw->wc", slot_table, gate_each).astype(jnp.bfloat16)
    got_grad, got_gate = (
        lax.all_to_all(sent_grad, "expert", split_axis=0, concat_axis=0, tiled=True),
        lax.all_to_all(sent_gate, "expert", split_axis=0, concat_axis=0, tiled=True),
    )
    slot_rows = got_grad.reshape(sources * capacity, width)
    gate_flat = got_gate.reshape(sources * capacity).astype(jnp.float32)
    weight_now = down_weight[0]
    raw_grad = lax.dot_general(
        slot_rows, weight_now, (((1,), (1,)), ((), ())), preferred_element_type=jnp.float32
    )
    hidden_flat = saved_hidden[0, 0].reshape(sources * capacity, hidden_units)
    hid_grad = (gate_flat[:, None] * raw_grad).astype(jnp.bfloat16)
    scores = jnp.sum(raw_grad * hidden_flat.astype(jnp.float32), axis=1).reshape(sources, capacity)
    scaled = (gate_flat[:, None] * slot_rows.astype(jnp.float32)).astype(jnp.bfloat16)
    down_grad = lax.psum_scatter(
        lax.dot_general(
            hidden_flat, scaled, (((0,), (0,)), ((), ())), preferred_element_type=jnp.float32
        ).astype(jnp.bfloat16),
        "dp",
        scatter_dimension=0,
        tiled=True,
    ).astype(jnp.float32)
    returned = lax.all_to_all(scores, "expert", split_axis=0, concat_axis=0, tiled=True)
    per_token = jnp.einsum("wct,wc->tw", slot_table, returned)
    score_tok = jnp.einsum("tkw,tw->tk", hit_mask, per_token)
    score_all = jnp.where(expert_ids < window, score_tok, rest_scores)
    mean_part = jnp.sum(gate_sel * score_all, axis=1, keepdims=True)
    logit_sel = gate_sel * (score_all - mean_part)
    logit_bf = jnp.einsum("tke,tk->te", all_mask, logit_sel).astype(jnp.bfloat16)
    summed_rows = lax.psum_scatter(
        lax.dot_general(
            tokens_in, logit_bf, (((0,), (0,)), ((), ())), preferred_element_type=jnp.float32
        ).astype(jnp.bfloat16),
        "dp",
        scatter_dimension=0,
        tiled=True,
    )
    router_grad = lax.psum_scatter(summed_rows, "expert", scatter_dimension=1, tiled=True).astype(
        jnp.float32
    )
    token_grad = lax.dot_general(
        logit_bf, router_weight, (((1,), (1,)), ((), ())), preferred_element_type=jnp.float32
    ).astype(jnp.bfloat16)
    hidden_grad = hid_grad.reshape(1, 1, sources, capacity, hidden_units)
    return (token_grad, router_grad, down_grad[None], hidden_grad)


MESH = pl.DeviceIdType.MESH
F32, BF16 = jnp.float32, jnp.bfloat16


def flip(index, mask):
    out = 0
    for bit in (1, 2, 4):
        digit = lax.rem(lax.div(index, bit), 2)
        out = out + bit * ((1 - digit) if mask & bit else digit)
    return out


def rows_times(a, b):
    return lax.dot_general(a, b, (((1,), (1,)), ((), ())), preferred_element_type=F32)


def times(a, b):
    return lax.dot_general(a, b, (((1,), (0,)), ((), ())), preferred_element_type=F32)


def down_part(group, gat, hg_all, cols):
    lhs = jnp.concatenate([hg_all[j] for j in group], axis=1)
    slots = lhs.shape[1] // len(group)
    rhs = jnp.concatenate([gat[j, :, :, cols].reshape(slots, -1) for j in group], axis=0)
    return times(lhs, rhs)


def layer_kernel(
    nd, nz, cap,
    tok_h, grad_h, ids_h, rest_h, rw_h, w_h, hid_h,
    token_o, router_o, down_o, hidden_o, gat, hg_all,
    tok, grad, ids, rest, rw, weight, hid,
    blk, y, gate_s, gate_r, ret_s, ret_r, tok_all, info_s, info_all, sc_s, sc_all,
    gate_all, base_all, hg_s, rg_s, rg_r,
    load_sem, send_sem, recv_sem, disp_r, near_r, in_r,
):
    me = lax.axis_index("dp")
    mz = lax.axis_index("expert")
    tokens, width = tok.shape
    experts = rw.shape[1]
    slots = nz * cap
    hidden_units = hid.shape[1]
    own_cols = width // nd

    loads = []
    for i, (src, dst) in enumerate(
        ((ids_h, ids), (grad_h, grad), (tok_h, tok), (rw_h, rw), (rest_h, rest), (hid_h, hid), (w_h, weight))
    ):
        loads.append(pltpu.make_async_copy(src, dst, load_sem.at[i]))
        loads[-1].start()
    ld_ids, ld_grad, ld_tok, ld_rw, ld_rest, ld_hid, ld_w = loads
    disp_s, gsem_s, ag_s, tk_s, rs_s, in_s, st_s, hs_s, zr_s = [send_sem.at[i] for i in range(9)]
    gsem_r, tk_r, rs_r, ina_r, st_r, hs_r, zr_r, core_r, last_r = [recv_sem.at[i] for i in range(9)]
    peers = [flip(me, p) for p in range(nd)]
    half = lax.div(mz, 2)
    near = [mz, mz + 1 - 2 * lax.rem(mz, 2), 2 - half, 3 - 3 * half]
    barrier = pltpu.get_barrier_semaphore()
    for p in range(1, nd):
        pl.semaphore_signal(barrier, inc=1, device_id=(peers[p], mz), device_id_type=MESH)
    for k in range(1, nz):
        pl.semaphore_signal(barrier, inc=1, device_id=(me, near[k]), device_id_type=MESH)


    def send(src, dst, s_sem, r_sem, device):
        pltpu.make_async_remote_copy(
            src_ref=src, dst_ref=dst, send_sem=s_sem, recv_sem=r_sem, device_id=device, device_id_type=MESH
        ).start()

    def arrived(ref, r_sem):
        pltpu.make_async_copy(ref, ref, r_sem).wait()

    e_row = lax.broadcasted_iota(jnp.int32, (experts, tokens), 0)
    ld_ids.wait()
    idv = ids[...]
    topk = idv.shape[0]
    hits = [idv[k : k + 1, :] == e_row for k in range(topk)]
    mask = hits[0]
    for k in range(1, topk):
        mask = mask | hits[k]
    t_row = lax.broadcasted_iota(jnp.int32, (tokens, tokens), 0)
    t_col = lax.broadcasted_iota(jnp.int32, (tokens, tokens), 1)
    earlier = jnp.where(t_row < t_col, 1.0, 0.0).astype(BF16)
    chosen = jnp.where(mask, 1.0, 0.0)
    place = jnp.where(mask, times(chosen.astype(BF16), earlier), -1.0)
    c_row = lax.broadcasted_iota(jnp.int32, (cap, tokens), 0).astype(F32)
    tables = [jnp.where(place[e : e + 1, :] == c_row, 1.0, 0.0) for e in range(nz)]
    table = jnp.concatenate(tables, axis=0).astype(BF16)

    ld_grad.wait()
    blk[...] = times(table, grad[...]).astype(BF16).reshape(blk.shape)
    gat[me, mz] = blk[mz]

    pl.semaphore_wait(barrier, nd - 1 + nz - 1)
    for k in Z_ORDER:
        send(blk.at[near[k]], gat.at[me, mz], disp_s, disp_r.at[mz], (me, near[k]))

    def pieces(k):
        parts = 2 if k in SPLIT else 1
        return [(h, pl.ds(h * (width // parts), width // parts)) for h in range(parts)]

    def via_of(k, h):
        return 4 if (k + h) % 2 else 2

    def near_sem(k, origin, h):
        return near_r.at[SLOT[k, origin, h]]

    def spread(k, h, cols, origin, target):
        from_p = origin ^ target
        ref = gat.at[peers[origin], near[k], :, cols]
        if from_p % 2 == 0:
            r_sem = near_sem(k, from_p, h)
        else:
            r_sem = last_r if from_p == 7 else core_r
        send(ref, ref, ag_s, r_sem, (peers[target], mz))

    def landed(k):
        arrived(gat.at[me, near[k]], disp_r.at[near[k]])

    def spread_own(k):
        for h, cols in pieces(k):
            via = via_of(k, h)
            for target in (via, 6 - via):
                spread(k, h, cols, 0, target)
        for h, cols in pieces(k):
            spread(k, h, cols, 0, 1)

    def relay_via(k, h):
        cols = pieces(k)[h][1]
        via = via_of(k, h)
        arrived(gat.at[peers[via], near[k], :, cols], near_sem(k, via, h))
        spread(k, h, cols, via, 6 - via)
        spread(k, h, cols, via, 1)

    def relay_core(k, h, origin):
        cols = pieces(k)[h][1]
        arrived(gat.at[peers[origin], near[k], :, cols], near_sem(k, origin, h))
        spread(k, h, cols, origin, 1)

    spread_own(0)

    ld_tok.wait()
    ld_rw.wait()
    logits = times(tok[...], rw[...]).T
    low = jnp.where(mask, logits, -3.0e38)
    raised = jnp.where(mask, jnp.exp(low - jnp.max(low, axis=0, keepdims=True)), 0.0)
    gate = raised / jnp.sum(raised, axis=0, keepdims=True)
    for k in range(topk):
        info_s[k : k + 1, :] = jnp.sum(jnp.where(hits[k], gate, 0.0), axis=0, keepdims=True)
    ld_rest.wait()
    restv = rest[...]
    info_s[topk : 2 * topk, :] = restv
    info_s[2 * topk : 3 * topk, :] = idv.astype(F32)
    for e in range(nz):
        one = jnp.sum(tables[e] * gate[e : e + 1, :], axis=1, keepdims=True)
        gate_s[e] = jnp.broadcast_to(one, (cap, experts)).astype(BF16)
    gate_r[mz] = gate_s[mz]
    for k in range(1, nz):
        send(gate_s.at[near[k]], gate_r.at[mz], gsem_s, gsem_r, (me, near[k]))
    for p in (6, 2, 4, 1):
        send(info_s, info_all.at[me], in_s, in_r.at[p // 2] if p > 1 else ina_r, (peers[p], mz))
    def send_tokens(p):
        cols = pl.ds(pl.multiple_of(peers[p] * own_cols, own_cols), own_cols)
        send(tok.at[:, cols], tok_all.at[me], tk_s, tk_r, (peers[p], mz))

    for p in EARLY_TOKENS:
        send_tokens(p)

    ld_hid.wait()
    ld_w.wait()
    y[...] = times(hid[...], weight[...]).reshape(y.shape)

    outside = e_row >= nz

    def expand(j, g, r):
        r = jnp.where(outside, r, 0.0)
        gate_all[j] = g
        base_all[j] = g * (r - jnp.sum(g * r, axis=0, keepdims=True))

    rest_all = jnp.where(hits[0], restv[0:1, :], 0.0)
    for k in range(1, topk):
        rest_all = jnp.where(hits[k], restv[k : k + 1, :], rest_all)
    expand(me, gate, rest_all)
    tok_all[me] = tok[:, pl.ds(pl.multiple_of(me * own_cols, own_cols), own_cols)]

    def score_of(k):
        score = jnp.sum(gat[me, near[k]].astype(F32) * y[near[k]], axis=1, keepdims=True)
        target = ret_s if k else ret_r
        target[near[k]] = jnp.broadcast_to(score, (cap, tokens))
        if k:
            send(ret_s.at[near[k]], ret_r.at[mz], rs_s, rs_r, (me, near[k]))

    def logit_grad(j, score):
        g = gate_all[j]
        mean = jnp.sum(g[0:nz, :] * score, axis=0, keepdims=True)
        late = base_all[j] - g * mean
        for e in range(nz):
            late = late + jnp.where(e_row == e, g * score[e : e + 1, :], 0.0)
        return late

    def hidden_part(n, parts):
        step = hidden_units // parts
        slot_g = gate_r[...].reshape(slots, experts)[:, 0:1].astype(F32)
        raw = rows_times(gat[me].reshape(slots, width), weight[n * step : (n + 1) * step, :])
        hidden_o[:, n * step : (n + 1) * step] = (slot_g * raw).astype(BF16)

    def gates_in():
        arrived(gate_r.at[1:nz], gsem_r)
        slot_g = gate_r[...].reshape(slots, experts)[:, 0:1].astype(F32)
        hidden_f = hid[...].astype(F32)
        scaled_t = (slot_g * hidden_f).T.astype(BF16)
        hg_s[...] = scaled_t.reshape(hg_s.shape)
        hg_all[me] = hg_s[me]

    def facts_on():
        for p in (2, 4, 6):
            ref = info_all.at[peers[p]]
            arrived(ref, in_r.at[p // 2])
            send(ref, ref, in_s, ina_r, (peers[1], mz))

    def facts_in():
        e_rowf = e_row.astype(F32)
        for p in (2, 4, 6, 1, 3, 5, 7):
            j = peers[p]
            if p == 1:
                arrived(info_all.at[0:4], ina_r)
            g = jnp.zeros((experts, tokens), F32)
            r = g
            for k in range(topk):
                hit = info_all[j, 2 * topk + k : 2 * topk + k + 1, :] == e_rowf
                g = jnp.where(hit, info_all[j, k : k + 1, :], g)
                r = jnp.where(hit, info_all[j, topk + k : topk + k + 1, :], r)
            expand(j, g, r)

    def scores_out():
        arrived(ret_r.at[1:nz], rs_r)
        for e in range(nz):
            sc_s[e : e + 1, :] = jnp.sum(tables[e] * ret_r[e], axis=0, keepdims=True)
        for p in TOKEN_ORDER:
            send(sc_s, sc_all.at[me], st_s, st_r, (peers[p], mz))

    def hidden_out():
        for p in TOKEN_ORDER:
            send(hg_s.at[peers[p]], hg_all.at[me], hs_s, hs_r, (peers[p], mz))

    def token_part():
        own_grad = logit_grad(me, sc_s[0:nz, :])
        token_o[...] = rows_times(own_grad.T.astype(BF16), rw[...]).astype(BF16)

    def router_part():
        arrived(sc_all.at[1:nd], st_r)
        grads = [logit_grad(me, sc_s[0:nz, :]).astype(BF16)]
        for p in range(1, nd):
            grads.append(logit_grad(peers[p], sc_all[peers[p], 0:nz, :]).astype(BF16))
        arrived(tok_all.at[1:nd], tk_r)
        lhs = jnp.concatenate(grads, axis=1)
        rhs = jnp.concatenate([tok_all[peers[p]] for p in range(nd)], axis=0)
        partial = times(lhs, rhs)
        rg_s[...] = partial.reshape(rg_s.shape).astype(BF16)
        rg_r[mz] = rg_s[mz]
        for k in Z_ORDER:
            send(rg_s.at[near[k]], rg_r.at[mz], zr_s, zr_r, (me, near[k]))

    score_of(0)
    landed(1)
    score_of(1)
    spread_own(1)
    relay_via(0, 0)
    relay_via(0, 1)
    relay_core(0, 0, 6 - via_of(0, 0))
    relay_core(0, 1, 6 - via_of(0, 1))
    landed(2)
    score_of(2)
    spread_own(2)
    landed(3)
    score_of(3)
    facts_on()
    gates_in()
    hidden_part(0, 3)
    hidden_part(1, 3)
    scores_out()
    spread_own(3)
    hidden_out()
    relay_via(1, 0)
    relay_via(1, 1)
    relay_core(1, 0, 6 - via_of(1, 0))
    relay_core(1, 1, 6 - via_of(1, 1))
    relay_core(0, 0, 6)
    relay_core(0, 1, 6)
    facts_in()
    relay_via(2, 0)
    relay_via(2, 1)
    relay_core(2, 0, 6 - via_of(2, 0))
    relay_core(2, 1, 6 - via_of(2, 1))
    hidden_part(2, 3)
    router_part()
    relay_via(3, 0)
    relay_via(3, 1)
    relay_core(3, 0, 6 - via_of(3, 0))
    relay_core(3, 1, 6 - via_of(3, 1))
    relay_core(1, 0, 6)
    relay_core(1, 1, 6)
    relay_core(2, 0, 6)
    relay_core(2, 1, 6)
    token_part()
    relay_core(3, 0, 6)
    relay_core(3, 1, 6)
    arrived(hg_all.at[1:nd], hs_r)
    arrived(gat.at[0:3], core_r)

    step = width // 4
    for n in range(4):
        cols = slice(n * step, (n + 1) * step)
        down_o[:, cols] = down_part(peers[0 : nd // 2], gat, hg_all, cols)
    arrived(gat.at[0], last_r)
    arrived(rg_r.at[1:nz], zr_r)
    total = rg_r[0].astype(F32)
    for k in range(1, nz):
        total = total + rg_r[k].astype(F32)
    router_o[...] = total
    arrived(blk.at[1:nz], disp_s)
    arrived(gate_s.at[1:nz], gsem_s)
    arrived(gat.at[1:nd], ag_s)
    arrived(tok_all.at[1:nd], tk_s)
    arrived(ret_s.at[1:nz], rs_s)
    arrived(info_all.at[1:nd], in_s)
    arrived(sc_all.at[1:nd], st_s)
    arrived(hg_s.at[1:nd], hs_s)
    arrived(rg_s.at[1:nz], zr_s)


def out_kernel(nd, token, router, down, hidden, gat, hg_all, token_h, router_h, down_h, hidden_h, total, sem):
    copies = []

    def put(src, dst):
        copies.append(pltpu.make_async_copy(src, dst, sem.at[len(copies)]))
        copies[-1].start()

    put(token, token_h)
    put(hidden, hidden_h)
    put(router, router_h)
    me = lax.axis_index("dp")
    group = [flip(me, p) for p in range(nd // 2, nd)]
    step = down.shape[1] // DOWN_STEPS
    for n in range(DOWN_STEPS):
        cols = slice(n * step, (n + 1) * step)
        total[:, cols] = down[:, cols] + down_part(group, gat, hg_all, cols)
        put(total.at[:, cols], down_h.at[:, cols])
    for copy in copies:
        copy.wait()


def hand_out(nd, results):
    count = 4
    return pl.pallas_call(
        functools.partial(out_kernel, nd),
        out_shape=tuple(jax.ShapeDtypeStruct(r.shape, r.dtype) for r in results[:count]),
        in_specs=[pl.BlockSpec(memory_space=pltpu.VMEM)] * len(results),
        out_specs=(pl.BlockSpec(memory_space=pltpu.HBM),) * count,
        scratch_shapes=[
            pltpu.VMEM(results[2].shape, results[2].dtype), pltpu.SemaphoreType.DMA((3 + DOWN_STEPS,))
        ],
        compiler_params=pltpu.CompilerParams(vmem_limit_bytes=2**23),
    )(*results)


DOWN_STEPS = 4
VMEM_BYTES = 67043328
TOKEN_ORDER = (6, 7, 2, 4, 3, 5, 1)
Z_ORDER = (3, 2, 1)
EARLY_TOKENS = (1, 7, 2, 4, 3, 5, 6)
SPLIT = (0, 1, 2, 3)
SLOT = {}
for piece in range(4):
    for place in (2, 4, 6):
        for part in range(2 if piece in SPLIT else 1):
            SLOT[piece, place, part] = len(SLOT)


def fused(nd, nz, tokens_in, out_grad, expert_ids, rest_scores, router_weight, down_weight, saved_hidden):
    cap, hidden_units = saved_hidden.shape[3], saved_hidden.shape[4]
    sources = saved_hidden.shape[2]
    tokens, width = tokens_in.shape
    experts = router_weight.shape[1]
    topk = expert_ids.shape[1]
    slots = sources * cap
    own_rows, own_cols, own_exp = hidden_units // nd, width // nd, experts // nz
    vm, dma = pltpu.VMEM, pltpu.SemaphoreType.DMA
    scratch = [
        vm((tokens, width), BF16), vm((tokens, width), BF16),
        vm(expert_ids.shape[::-1], jnp.int32), vm(rest_scores.shape[::-1], F32),
        vm((width, experts), BF16), vm((hidden_units, width), BF16), vm((slots, hidden_units), BF16),
        vm((nz, cap, width), BF16), vm((nz, cap, width), F32),
        vm((nz, cap, experts), BF16), vm((nz, cap, experts), BF16),
        vm((nz, cap, tokens), F32), vm((nz, cap, tokens), F32),
        vm((nd, tokens, own_cols), BF16),
        vm((3 * topk, tokens), F32), vm((nd, 3 * topk, tokens), F32),
        vm((nz, tokens), F32), vm((nd, nz, tokens), F32),
        vm((nd, experts, tokens), F32), vm((nd, experts, tokens), F32),
        vm((nd, own_rows, slots), BF16),
        vm((nz, own_exp, own_cols), BF16), vm((nz, own_exp, own_cols), BF16),
        dma((7,)), dma((9,)), dma((9,)), dma((nz,)), dma((len(SLOT),)), dma((nz,)),
    ]
    vm_spec = pl.BlockSpec(memory_space=pltpu.VMEM)
    held = 2 * tokens * width + 4 * own_exp * own_cols + 4 * own_rows * width + 2 * slots * hidden_units
    held = held + 2 * nd * slots * width + 2 * nd * own_rows * 128
    results = pl.pallas_call(
        functools.partial(layer_kernel, nd, nz, cap),
        out_shape=(
            pltpu.VMEM((tokens, width), BF16),
            pltpu.VMEM((own_exp, own_cols), F32),
            pltpu.VMEM((own_rows, width), F32),
            pltpu.VMEM((slots, hidden_units), BF16),
            pltpu.VMEM((nd, nz, cap, width), BF16),
            pltpu.VMEM((nd, own_rows, slots), BF16),
        ),
        in_specs=[pl.BlockSpec(memory_space=pltpu.HBM)] * 7,
        out_specs=(vm_spec,) * 6,
        scratch_shapes=scratch,
        compiler_params=pltpu.CompilerParams(
            collective_id=0, has_side_effects=True, vmem_limit_bytes=VMEM_BYTES - held
        ),
    )(
        tokens_in, out_grad, expert_ids.T, rest_scores.T, router_weight,
        down_weight[0], saved_hidden.reshape(slots, hidden_units),
    )
    token_grad, router_grad, down_grad, hidden_grad = hand_out(nd, results)
    return token_grad, router_grad.T, down_grad[None], hidden_grad.reshape(saved_hidden.shape)


def body(nd, nz, *args):
    tokens_in, saved_hidden, router_weight = args[0], args[6], args[4]
    slots = saved_hidden.shape[2] * saved_hidden.shape[3]
    gathered = nd * slots * tokens_in.shape[1] * 2
    fits = nd == 8 and gathered <= 16 * 2**20 and saved_hidden.shape[2] == nz
    fits = fits and nz == 4 and (saved_hidden.shape[4] // nd) % 16 == 0
    if fits:
        return fused(nd, nz, *args)
    return shards(*args)


def solution(mesh):
    sizes = dict(mesh.shape)
    return jax.shard_map(
        functools.partial(body, sizes["dp"], sizes["expert"]),
        mesh=mesh,
        in_specs=(
            P(("dp", "expert"), None),
            P(("dp", "expert"), None),
            P(("dp", "expert"), None),
            P(("dp", "expert"), None),
            P(),
            P("expert", None, None),
            P("dp", "expert", None, None, None),
        ),
        out_specs=(
            P(("dp", "expert"), None),
            P("dp", "expert"),
            P("expert", "dp", None),
            P("dp", "expert", None, None, None),
        ),
        check_vma=False,
    )
```
